32 devices in a mesh: dp: 2 (over x), fsdp: 4 (over y, core), tensor: 4 (over z).
Axes of the slice: x: 2, y: 2, z: 4, core: 2. Of those that a mesh axis runs over, the one named last changes fastest.
Arguments:
- hidden: bfloat16 [4096, 2048], P(('dp', 'fsdp'), 'tensor'), may hold values from -8 to 8
- norm_gain: bfloat16 [2048], P('tensor'), may hold values from 0.099609375 to 1.8984375
- head_weight: bfloat16 [2048, 32128], P('fsdp', 'tensor'), may hold values from -1 to 1
- token_ids: int32 [8, 512], P(('dp', 'fsdp')), may hold values from 0 to 32127
- lengths: int32 [8], P(('dp', 'fsdp')), may hold values from 128 to 512
- old_logp: float32 [8, 512], P(('dp', 'fsdp')), may hold values from -12.5 to -9.5
- advantages: float32 [8, 512], P(('dp', 'fsdp')), may hold values from -4 to 4
- rollout_logp: float32 [8, 512], P(('dp', 'fsdp'), 'tensor'), may hold values from -16 to -1
- rollout_row: int32 [8], P(('dp', 'fsdp')), may hold values from 0 to 7, each once
Outputs:
- new_logp: float32 [8, 512], P(('dp', 'fsdp'))
- token_loss: float32 [8, 512], P(('dp', 'fsdp'))
- summary: float32 [3], replicated
The draws below stay inside these ranges and needn't reach their ends.
Inputs may be any that keep to these rules, and one draw needn't show every extreme that they name: `rollout_row`: every row 0 to 7 is named once.
All inputs are finite; a program needn't handle non-finite values.
Results may differ from the reference program's by a relative error of at most 0.0005.
The reference program's roundings to bfloat16 on the way (of `normed`) count: a program that leaves them out, or rounds other values in their place, can miss the bound.
Values may be sent and summed in bfloat16 or wider, within the bound.
A program may use at most 128 MiB of HBM per device.

```python
import math
import jax
import jax.numpy as jnp
import numpy as np
from jax import lax

D = 2048
VOCAB = 32128
LEN = 512
RESP = 8
TOKENS = 4096


def draw_hidden(key, part):
    samples = jax.random.normal(jax.random.fold_in(key, 21), (TOKENS, D), jnp.float32)
    return jnp.clip(samples, -8.0, 8.0).astype(jnp.bfloat16)


def draw_head_weight(key, part):
    weights = jax.random.normal(jax.random.fold_in(key, 31), (D, VOCAB), jnp.float32) / math.sqrt(D)
    return jnp.clip(weights, -1.0, 1.0).astype(jnp.bfloat16)


def draw_lengths(key, part):
    row_index = jnp.arange(RESP, dtype=jnp.int32)
    shortest = LEN // 4
    rising = shortest + row_index * (LEN - shortest) // max(RESP - 1, 1)
    jitter = jax.random.randint(jax.random.fold_in(key, 41), (RESP,), 0, LEN // 8 + 1)
    values = jnp.clip(rising - jitter, shortest, LEN)
    values = jnp.where(row_index == RESP - 1, LEN, values)
    values = jnp.where(row_index == 0, shortest, values)
    return values.astype(jnp.int32)


def draw_rollout_logp(key, part):
    center = -math.log(VOCAB)
    row_offset = jax.random.uniform(jax.random.fold_in(key, 51), (RESP, 1), jnp.float32, -2.0, 2.0)
    token_jitter = jax.random.uniform(jax.random.fold_in(key, 52), (RESP, LEN), jnp.float32, -1.0, 1.0)
    return jnp.clip(center + row_offset + token_jitter, -16.0, -1.0)


def with_ends(array, rng, smallest, largest):
    longest = array.shape.index(max(array.shape))
    spots = []
    for shift in (0, 1):
        where = [jax.random.randint(jax.random.fold_in(rng, axis), (), 0, length) for axis, length in enumerate(array.shape)]
        where[longest] = (where[longest] + shift) % array.shape[longest]
        spots.append(tuple(where))
    return array.at[spots[0]].set(smallest).at[spots[1]].set(largest)


def block_levels(key, dims, cuts, low, high):
    loudness, own = 1.0, jax.random.fold_in(key, 6)
    for dim, parts in cuts:
        draws = jnp.exp(jax.random.uniform(jax.random.fold_in(own, dim), (parts,), jnp.float32, low / len(cuts), high / len(cuts)))
        loudness = loudness * jnp.repeat(draws, dims[dim] // parts).reshape([-1 if axis == dim else 1 for axis in range(len(dims))])
    return loudness


def cumulative_ranks(amount, slope):
    portions = [(1 << 20) // math.isqrt(rank ** slope) + 1 for rank in range(1, amount + 1)]
    deviation = 1 + sum(portions) // (1 << 30)
    return np.cumsum(np.array([max(1, weight // deviation) for weight in portions]))


def ranked_ids(stream_key, extent, amount, skew):
    listing = cumulative_ranks(amount, skew)
    lot = jax.random.randint(jax.random.fold_in(stream_key, 1), extent, 0, int(listing[amount - 1]))
    standing = jnp.searchsorted(jnp.asarray(listing, jnp.int32), lot, side="right")
    return jax.random.permutation(jax.random.fold_in(stream_key, 2), amount)[standing].astype(jnp.int32)


def noise(own_key, extent, deviation, most, cuts=(), kind=jnp.bfloat16):
    drawn = jax.random.normal(own_key, extent, jnp.float32) * deviation
    if len(cuts) > 0:
        drawn = block_levels(own_key, extent, cuts, -0.22, 0.18) * drawn
    return jnp.clip(drawn, min=-most, max=most).astype(kind)


def setup_inputs(seed: int = 0) -> dict:
    splits = jax.random.split(jax.random.key(seed), 10)
    hidden = draw_hidden(jax.random.fold_in(splits[9], 71), 0)
    norm_gain = jnp.clip(1.0 + 0.18 * jax.random.normal(splits[1], (D,), jnp.float32), 0.099609375, 1.8984375).astype(jnp.bfloat16)
    head_weight = draw_head_weight(jax.random.fold_in(splits[9], 71), 0)
    token_ids = with_ends(ranked_ids(splits[3], (RESP, LEN), VOCAB, 2), jax.random.fold_in(splits[3], 3), 0, VOCAB - 1).astype(jnp.int32)
    lengths = draw_lengths(jax.random.fold_in(splits[9], 71), 0)
    old_logp = jnp.clip(-12.5 + 3.0 * jax.random.uniform(splits[5], (RESP, LEN), jnp.float32) ** block_levels(splits[5], (RESP, LEN), ((0, 8),), -0.2, 0.2), -12.5, -9.5)
    advantages = noise(splits[6], (RESP, LEN), 1.0, 4.0, ((0, 8),), jnp.float32)
    rollout_logp = draw_rollout_logp(jax.random.fold_in(splits[9], 71), 0)
    rollout_row = jax.random.permutation(splits[8], RESP).astype(jnp.int32)
    return {"hidden": hidden, "norm_gain": norm_gain, "head_weight": head_weight, "token_ids": token_ids, "lengths": lengths, "old_logp": old_logp, "advantages": advantages, "rollout_logp": rollout_logp, "rollout_row": rollout_row}


clip_eps = 0.2
kl_coef = 0.2
log_limit = 10.0
norm_eps = 1e-06

def token_terms(new_logp, old_logp, advantages, ref_logp, live_mask, prob_square):
    shift = new_logp - old_logp
    prob_ratio = jnp.exp(jnp.clip(shift, -log_limit, log_limit))
    clipped = jnp.clip(prob_ratio, 1.0 - clip_eps, 1.0 + clip_eps)
    plain_term = prob_ratio * advantages
    bounded_term = clipped * advantages
    surrogate = jnp.minimum(plain_term, bounded_term)
    ref_gap = ref_logp - new_logp
    gap_clip = jnp.clip(ref_gap, -log_limit, log_limit)
    kl_term = jnp.exp(gap_clip) - gap_clip - 1.0
    token_loss = live_mask * (kl_coef * kl_term - surrogate)
    inside_gap = (jnp.abs(ref_gap) < log_limit).astype(jnp.float32)
    inside_ratio = (jnp.abs(shift) < log_limit).astype(jnp.float32)
    active_term = (plain_term <= bounded_term).astype(jnp.float32)
    grad_coef = live_mask * (kl_coef * (1.0 - jnp.exp(gap_clip)) * inside_gap - advantages * prob_ratio * active_term * inside_ratio)
    grad_square = grad_coef * grad_coef * (prob_square - 2.0 * jnp.exp(new_logp) + 1.0)
    return (token_loss, live_mask * kl_term, grad_square)

def reference(hidden, norm_gain, head_weight, token_ids, lengths, old_logp, advantages, rollout_logp, rollout_row):
    values = hidden.astype(jnp.float32)
    inv_rms = lax.rsqrt(lax.optimization_barrier(jnp.mean(values * values, axis=1, keepdims=True)) + norm_eps)
    normed = (values * inv_rms * norm_gain.astype(jnp.float32)[None, :]).astype(jnp.bfloat16)
    blocks = normed.reshape(token_ids.shape[0], token_ids.shape[1], normed.shape[1])

    def per_response(block):
        block_rows, block_ids = block
        logits = jnp.dot(block_rows, head_weight, preferred_element_type=jnp.float32)
        row_max = lax.optimization_barrier(jnp.max(logits, axis=1))
        shifted = jnp.exp(logits - row_max[:, None])
        exp_sum = lax.optimization_barrier(jnp.sum(shifted, axis=1))
        exp_square = lax.optimization_barrier(jnp.sum(shifted * shifted, axis=1))
        picked = jnp.take_along_axis(logits, block_ids[:, None].astype(jnp.int32), axis=1)[:, 0]
        return (picked - row_max - jnp.log(exp_sum), exp_square / (exp_sum * exp_sum))
    new_logp, prob_square = lax.map(per_response, (blocks, token_ids))
    ref_logp = jnp.take(rollout_logp, rollout_row.astype(jnp.int32), axis=0)
    positions = lax.broadcasted_iota(jnp.int32, token_ids.shape, 1)
    live_mask = (positions < lengths[:, None]).astype(jnp.float32)
    token_loss, kl_part, grad_part = token_terms(new_logp, old_logp, advantages, ref_logp, live_mask, prob_square)
    live_count = jnp.sum(live_mask)
    summary = jnp.stack([jnp.sum(token_loss) / live_count, jnp.sum(kl_part) / live_count, jnp.sqrt(jnp.sum(grad_part) / live_count)])
    return (new_logp, token_loss, summary)
```

```python
import functools

import jax
import jax.numpy as jnp
from jax import lax
from jax.experimental import pallas as pl
from jax.experimental.pallas import tpu as pltpu
from jax.sharding import PartitionSpec as P

MESH = pl.DeviceIdType.MESH
clip_eps = 0.2
kl_coef = 0.2
log_limit = 10.0
norm_eps = 1e-06
LANES = 128
LOW = -1e30


def token_terms(new_logp, old_logp, advantages, ref_logp, live_mask, prob_square):
    shift = new_logp - old_logp
    prob_ratio = jnp.exp(jnp.clip(shift, -log_limit, log_limit))
    clipped = jnp.clip(prob_ratio, 1.0 - clip_eps, 1.0 + clip_eps)
    plain_term = prob_ratio * advantages
    bounded_term = clipped * advantages
    surrogate = jnp.minimum(plain_term, bounded_term)
    ref_gap = ref_logp - new_logp
    gap_clip = jnp.clip(ref_gap, -log_limit, log_limit)
    gap_exp = jnp.exp(gap_clip)
    kl_term = gap_exp - gap_clip - 1.0
    token_loss = live_mask * (kl_coef * kl_term - surrogate)
    gap_part = jnp.where(jnp.abs(ref_gap) < log_limit, kl_coef * (1.0 - gap_exp), 0.0)
    active = (plain_term <= bounded_term) & (jnp.abs(shift) < log_limit)
    grad_coef = live_mask * (gap_part - jnp.where(active, plain_term, 0.0))
    grad_square = grad_coef * grad_coef * (prob_square - 2.0 * jnp.exp(new_logp) + 1.0)
    return (token_loss, live_mask * kl_term, grad_square)


class Config:
    def __init__(self, mesh, tok, dz, kr, vt):
        self.dp, self.fs, self.tz = (mesh.shape[a] for a in ("dp", "fsdp", "tensor"))
        self.groups = self.fs // 2
        self.tok, self.dz, self.kr, self.vt = tok, dz, kr, vt
        self.dim = dz * self.tz
        self.full_tiles = vt // LANES
        tiles = -(-vt // LANES)
        self.half_tiles = -(-tiles // (self.groups * self.dp))
        self.half_cols = self.half_tiles * LANES
        self.block_cols = self.half_cols * self.dp
        self.pad_cols = self.block_cols * self.groups
        self.steps = 8
        self.rows = tok // self.steps
        self.chunk = 256 if self.half_cols % 256 == 0 else LANES
        self.wsteps = self.half_cols // self.chunk
        self.resp = self.dp * self.fs


def kernel(
    c,
    hid, w_any, tail_any, pack_in, ids_in, old_in, adv_in, len_in, row_in,
    logp_out, loss_out, sum_out,
    x_buf, n_buf, w_own, w_full, packs, ids_all, rel, m_buf, l_buf, q_buf, p_buf,
    row_buf, roll, s_out, s_in, t_out, t_in,
    load_sem, x_sem, own_sem, tok_recv, y_send, right_send, left_send,
    wy_send, wy_recv, wx_send, wx_recv, core_send, core_recv,
    ids_send, ids_recv, pack_send, pack_recv, roll_send, roll_recv,
    st_send, st_recv, tot_send, tot_recv,
):
    G, Z, DP, F = c.groups, c.tz, c.dp, c.fs
    x = lax.axis_index("dp")
    f = lax.axis_index("fsdp")
    z = lax.axis_index("tensor")
    g, core = f // 2, f % 2
    partner = (x, g * 2 + (1 - core), z)
    me_resp = x * F + f
    pending = []

    def dev_g(gi):
        return (x, gi * 2 + core, z)

    def dev_x(xi):
        return (xi, f, z)

    def dev_z(zi):
        return (x, f, zi)

    def group(d):
        return lax.rem(g + d, G)

    def remote(src, dst, ss, rs, dev):
        return pltpu.make_async_remote_copy(
            src_ref=src, dst_ref=dst, send_sem=ss, recv_sem=rs, device_id=dev, device_id_type=MESH
        )

    def send(src, dst, ss, rs, dev, cond=None):
        copy = remote(src, dst, ss, rs, dev)
        if cond is None:
            copy.start()
        else:
            pl.when(cond)(copy.start)
        pending.append((cond, copy))

    def arrive(dst, rs, cond=None):
        copy = remote(dst, dst, rs, rs, partner)
        if cond is None:
            copy.wait_recv()
        else:
            pl.when(cond)(copy.wait_recv)

    main_cols = c.full_tiles * LANES
    loads = [
        pltpu.make_async_copy(
            w_any.at[:, pl.ds(0, main_cols)], w_own.at[:, pl.ds(0, main_cols)], load_sem.at[0]
        )
    ]
    if main_cols < c.vt:
        loads.append(
            pltpu.make_async_copy(tail_any, w_own.at[:, pl.ds(main_cols, LANES)], load_sem.at[1])
        )
    for copy in loads:
        copy.start()
    zcols = pl.ds(pl.multiple_of(z * c.dz, c.dz), c.dz)
    own_x = pltpu.make_async_copy(hid, x_buf.at[g, :, zcols], x_sem)
    own_x.start()
    filled = min(-(-c.vt // LANES) * LANES, c.pad_cols)
    if filled < c.pad_cols:
        w_own[:, filled:] = jnp.zeros((c.kr, c.pad_cols - filled), w_own.dtype)

    barrier = pltpu.get_barrier_semaphore()
    count = 0
    for dg in range(G):
        for s in range(Z):
            if dg or s:
                pl.semaphore_signal(
                    barrier, inc=1,
                    device_id=(x, group(dg) * 2 + core, lax.rem(z + s, Z)), device_id_type=MESH,
                )
                count += 1
    for dx in range(DP):
        for df in range(F):
            if dx or df % 2:
                pl.semaphore_signal(
                    barrier, inc=1,
                    device_id=(lax.rem(x + dx, DP), lax.rem(f + df, F), z), device_id_type=MESH,
                )
                count += 1
    pl.semaphore_wait(barrier, count)

    def piece(gi, q, zi):
        return x_buf.at[
            gi, pl.ds(q * c.rows, c.rows), pl.ds(pl.multiple_of(zi * c.dz, c.dz), c.dz)
        ]

    def hid_piece(q):
        return hid.at[pl.ds(q * c.rows, c.rows), :]

    def w_block(fi, h, j):
        return w_full.at[
            pl.ds(pl.multiple_of(fi * c.kr, c.kr), c.kr),
            pl.ds(pl.multiple_of(h * c.half_cols + j * c.chunk, c.chunk), c.chunk),
        ]

    def own_block(gi, h, j):
        start = gi * c.block_cols + h * c.half_cols + j * c.chunk
        return w_own.at[:, pl.ds(pl.multiple_of(start, c.chunk), c.chunk)]

    def y_tokens(q):
        for d in range(1, G):
            send(hid_piece(q), piece(g, q, z), y_send.at[d, q], tok_recv.at[g, q, z], dev_g(group(d)))

    def y_weights(j):
        for d in range(1, G):
            gi = group(d)
            send(own_block(gi, x, j), w_block(f, x, j), wy_send.at[d, j], wy_recv.at[g, j], dev_g(gi))

    def z_move(q, s):
        right_ok = z - s >= 0
        left_ok = z + s < Z
        zr = jnp.maximum(z - s, 0)
        zl = jnp.minimum(z + s, Z - 1)
        for d in range(G):
            gi = group(d)
            if s == 0:
                if d:
                    arrive(piece(gi, q, z), tok_recv.at[gi, q, z])
                src_r = src_l = hid_piece(q) if d == 0 else piece(gi, q, z)
            else:
                arrive(piece(gi, q, zr), tok_recv.at[gi, q, zr], right_ok)
                arrive(piece(gi, q, zl), tok_recv.at[gi, q, zl], left_ok)
                src_r, src_l = piece(gi, q, zr), piece(gi, q, zl)
            if s < Z - 1:
                send(src_r, piece(gi, q, zr), right_send.at[gi, q, zr], tok_recv.at[gi, q, zr],
                     dev_z(jnp.minimum(z + 1, Z - 1)), right_ok & (z + 1 < Z))
                send(src_l, piece(gi, q, zl), left_send.at[gi, q, zl], tok_recv.at[gi, q, zl],
                     dev_z(jnp.maximum(z - 1, 0)), left_ok & (z >= 1))

    def core_pass(src, fi, h, j):
        gi = fi // 2
        send(src, w_block(fi, h, j), core_send.at[gi, h, j], core_recv.at[gi, h, j], partner)

    for d in range(1, G):
        send(ids_in, ids_all.at[g], ids_send.at[d], ids_recv.at[g], dev_g(group(d)))
    for s in range(1, Z):
        send(pack_in, packs.at[z], pack_send.at[s], pack_recv.at[z], dev_z(lax.rem(z + s, Z)))
    y_tokens(0)
    z_first = 0

    for gi_init in range(G):
        m_buf[gi_init] = jnp.full(m_buf.shape[1:], LOW, jnp.float32)
        for ref in (l_buf, q_buf, p_buf):
            ref[gi_init] = jnp.zeros(ref.shape[1:], jnp.float32)
    packs[z] = pack_in[...]
    ids_all[g] = ids_in[...]
    for copy in loads:
        copy.wait()
    y_weights(0)
    own_copies = []
    for h in range(DP):
        start = pl.multiple_of(g * c.block_cols + h * c.half_cols, LANES)
        copy = pltpu.make_async_copy(
            w_own.at[:, pl.ds(start, c.half_cols)],
            w_full.at[pl.ds(pl.multiple_of(f * c.kr, c.kr), c.kr), pl.ds(h * c.half_cols, c.half_cols)],
            own_sem.at[h],
        )
        copy.start()
        own_copies.append(copy)

    def normalize(q):
        rows = pl.ds(q * c.rows, c.rows)
        for gi in range(G):
            values = x_buf[gi, rows, :].astype(jnp.float32)
            inv = lax.rsqrt(jnp.sum(values * values, axis=1, keepdims=True) / c.dim + norm_eps)
            for zi in range(Z):
                gain = packs[zi, 0:1, 0:c.dz]
                part = values[:, zi * c.dz : (zi + 1) * c.dz]
                n_buf[gi, rows, zi * c.dz : (zi + 1) * c.dz] = (part * inv * gain).astype(jnp.bfloat16)

    lane = lax.broadcasted_iota(jnp.int32, (1, LANES), 1)

    def unit(q, j):
        rows = pl.ds(pl.multiple_of(q * c.rows, c.rows), c.rows)
        for h in range(DP):
            off = h * c.half_cols + j * c.chunk
            cols = pl.ds(pl.multiple_of(off, c.chunk), c.chunk)
            tokens = jnp.concatenate([n_buf[gi, rows, :] for gi in range(G)], axis=0)
            logits = jnp.dot(tokens, w_full[:, cols], preferred_element_type=jnp.float32)
            valid = c.vt - g * c.block_cols - off
            for gi in range(G):
                part = logits[gi * c.rows : (gi + 1) * c.rows]
                place = rel[gi, rows, :] - off
                parts = []
                picked = p_buf[gi, rows, :]
                for t in range(c.chunk // LANES):
                    col = part[:, t * LANES : (t + 1) * LANES]
                    picked = picked + jnp.where(place == t * LANES, col, 0.0)
                    parts.append(jnp.where(lane + t * LANES < valid, col, LOW))
                p_buf[gi, rows, :] = picked
                before = m_buf[gi, rows, :]
                top = before
                for col in parts:
                    top = jnp.maximum(top, col)
                scale = jnp.exp(before - top)
                total = l_buf[gi, rows, :] * scale
                square = q_buf[gi, rows, :] * (scale * scale)
                for col in parts:
                    e = jnp.exp(col - top)
                    total = total + e
                    square = square + e * e
                m_buf[gi, rows, :] = top
                l_buf[gi, rows, :] = total
                q_buf[gi, rows, :] = square

    for i in range(c.steps + Z - 1):
        if i + 1 < c.steps:
            y_tokens(i + 1)
        if i + 1 < c.wsteps:
            y_weights(i + 1)
        if i < c.wsteps:
            for h in range(DP):
                core_pass(own_block(g, h, i), f, h, i)
        if i < c.steps:
            z_move(i, 0)
        if 0 <= i - 1 < c.wsteps:
            j = i - 1
            for d in range(1, G):
                gi = group(d)
                fi = gi * 2 + core
                arrive(w_block(fi, x, j), wy_recv.at[gi, j])
                for dx in range(1, DP):
                    xi = lax.rem(x + dx, DP)
                    send(w_block(fi, x, j), w_block(fi, x, j), wx_send.at[gi, dx, j],
                         wx_recv.at[gi, x, j], dev_x(xi))
                core_pass(w_block(fi, x, j), fi, x, j)
        for s in range(1, Z - 1):
            if 0 <= i - s < c.steps:
                z_move(i - s, s)
        if 0 <= i - 2 < c.wsteps:
            j = i - 2
            for d in range(1, G):
                gi = group(d)
                fi = gi * 2 + core
                for dx in range(1, DP):
                    xi = lax.rem(x + dx, DP)
                    arrive(w_block(fi, xi, j), wx_recv.at[gi, xi, j])
                    core_pass(w_block(fi, xi, j), fi, xi, j)
        if i == 1:
            for s in range(1, Z):
                zi = lax.rem(z + s, Z)
                arrive(packs.at[zi], pack_recv.at[zi])
            row_buf[...] = sum(packs[zi, :, c.dz :] for zi in range(Z))
            for d in range(1, G):
                arrive(ids_all.at[group(d)], ids_recv.at[group(d)])
            base = z * c.vt + g * c.block_cols
            for gi in range(G):
                spread = jnp.broadcast_to(ids_all[gi, 0:1, :], (LANES, c.tok))
                rel[gi] = spread.T.astype(jnp.int32) - base - lane
            own_x.wait()
            for copy in own_copies:
                copy.wait()
        if i == 2:
            for dx in range(DP):
                for df in range(F):
                    if dx or df:
                        xi, fi = lax.rem(x + dx, DP), lax.rem(f + df, F)
                        send(row_buf, roll.at[me_resp], roll_send.at[dx, df], roll_recv.at[me_resp],
                             (xi, fi, z))
        q = i - (Z - 1)
        if q >= 0:
            if q < c.wsteps:
                for gi in range(G):
                    for h in range(DP):
                        arrive(w_block(gi * 2 + 1 - core, h, q), core_recv.at[gi, h, q])
                if q:
                    pl.loop(0, q)(lambda qq, q=q: unit(qq, q))
            z_move(q, Z - 1)
            normalize(q)
            pl.loop(0, min(q + 1, c.wsteps))(lambda j, q=q: unit(q, j))

    for gi in range(G):
        m_t = m_buf[gi].T
        top = jnp.max(m_t, axis=0, keepdims=True)
        scale = jnp.exp(m_t - top)
        total = jnp.sum(l_buf[gi].T * scale, axis=0, keepdims=True)
        square = jnp.sum(q_buf[gi].T * (scale * scale), axis=0, keepdims=True)
        picked = jnp.sum(p_buf[gi].T, axis=0, keepdims=True)
        s_out[gi] = jnp.concatenate([top, total, square, picked, jnp.zeros((4, c.tok), jnp.float32)], axis=0)
    for s in range(Z - 1, -1, -1):
        for d in range(G):
            if s or d:
                gi, zi = group(d), lax.rem(z + s, Z)
                send(s_out.at[gi], s_in.at[g, z], st_send.at[d, s], st_recv.at[g, z],
                     (x, gi * 2 + core, zi))
    s_in[g, z] = s_out[g]

    roll[me_resp] = row_buf[...]
    for dx in range(DP):
        for df in range(F):
            if dx or df:
                r = lax.rem(x + dx, DP) * F + lax.rem(f + df, F)
                arrive(roll.at[r], roll_recv.at[r])
    ref = jnp.zeros((1, c.tok), jnp.float32)
    for r in range(c.resp):
        ref = ref + jnp.where(row_in[0] == r, roll[r, 0:1, :], 0.0)
    position = lax.broadcasted_iota(jnp.int32, (1, c.tok), 1)
    live = jnp.where(position < len_in[0], 1.0, 0.0)

    for s in range(Z):
        for d in range(G):
            if s or d:
                gi, zi = group(d), lax.rem(z + s, Z)
                arrive(s_in.at[gi, zi], st_recv.at[gi, zi])
    every = [(gi, zi) for gi in range(G) for zi in range(Z)]
    top = s_in[0, 0, 0:1, :]
    for gi, zi in every[1:]:
        top = jnp.maximum(top, s_in[gi, zi, 0:1, :])
    total = square = picked = jnp.zeros((1, c.tok), jnp.float32)
    for gi, zi in every:
        scale = jnp.exp(s_in[gi, zi, 0:1, :] - top)
        total = total + s_in[gi, zi, 1:2, :] * scale
        square = square + s_in[gi, zi, 2:3, :] * (scale * scale)
        picked = picked + s_in[gi, zi, 3:4, :]
    new_logp = picked - top - jnp.log(total)
    prob_square = square / (total * total)
    token_loss, kl_part, grad_part = token_terms(
        new_logp, old_in[...], adv_in[...], ref, live, prob_square
    )
    sums = [jnp.sum(v, axis=1, keepdims=True) for v in (live, token_loss, kl_part, grad_part)]
    t_out[...] = jnp.concatenate(
        [jnp.broadcast_to(v, (1, LANES)) for v in sums] + [jnp.zeros((4, LANES), jnp.float32)], axis=0
    )
    for dx in range(DP):
        for df in range(F):
            if dx or df:
                xi, fi = lax.rem(x + dx, DP), lax.rem(f + df, F)
                send(t_out, t_in.at[me_resp], tot_send.at[dx, df], tot_recv.at[me_resp], (xi, fi, z))
    t_in[me_resp] = t_out[...]
    logp_out[...] = new_logp
    loss_out[...] = token_loss
    for dx in range(DP):
        for df in range(F):
            if dx or df:
                r = lax.rem(x + dx, DP) * F + lax.rem(f + df, F)
                arrive(t_in.at[r], tot_recv.at[r])
    totals = sum(t_in[r] for r in range(c.resp))
    count = totals[0:1]
    sum_out[...] = jnp.concatenate(
        [totals[1:2] / count, totals[2:3] / count, jnp.sqrt(totals[3:4] / count), jnp.zeros((5, LANES), jnp.float32)],
        axis=0,
    )
    for cond, copy in pending:
        if cond is None:
            copy.wait_send()
        else:
            pl.when(cond)(copy.wait_send)


def shards(c_of, hidden, norm_gain, head_weight, token_ids, lengths, old_logp, advantages, rollout_logp, rollout_row):
    c = c_of(hidden.shape[0], hidden.shape[1], head_weight.shape[0], head_weight.shape[1])
    G, Z, DP, F = c.groups, c.tz, c.dp, c.fs
    z = lax.axis_index("tensor")
    main_cols = c.full_tiles * LANES
    tail = jnp.pad(head_weight[:, main_cols:], ((0, 0), (0, LANES - (c.vt - main_cols))))
    part = rollout_logp.shape[1]
    row = lax.dynamic_update_slice(jnp.zeros((1, c.tok), jnp.float32), rollout_logp, (0, z * part))
    pack = jnp.broadcast_to(
        jnp.concatenate([norm_gain.astype(jnp.float32)[None, :], row], axis=1), (8, c.dz + c.tok)
    )
    ids = jnp.broadcast_to(token_ids.astype(jnp.float32), (8, c.tok))
    vmem = pl.BlockSpec(memory_space=pltpu.VMEM)
    smem = pl.BlockSpec(memory_space=pltpu.SMEM)
    hbm = pl.BlockSpec(memory_space=pl.ANY)
    dma = lambda *shape: pltpu.SemaphoreType.DMA(shape)
    f32 = jnp.float32
    lanes = lambda dtype: pltpu.VMEM((G, c.tok, LANES), dtype)
    Q, J = c.steps, c.wsteps
    new_logp, token_loss, summary = pl.pallas_call(
        functools.partial(kernel, c),
        out_shape=(
            jax.ShapeDtypeStruct((1, c.tok), f32),
            jax.ShapeDtypeStruct((1, c.tok), f32),
            jax.ShapeDtypeStruct((8, LANES), f32),
        ),
        in_specs=[vmem, hbm, hbm, vmem, vmem, vmem, vmem, smem, smem],
        out_specs=(vmem, vmem, vmem),
        scratch_shapes=[
            pltpu.VMEM((G, c.tok, c.dim), jnp.bfloat16),
            pltpu.VMEM((G, c.tok, c.dim), jnp.bfloat16),
            pltpu.VMEM((c.kr, c.pad_cols), jnp.bfloat16),
            pltpu.VMEM((c.dim, c.block_cols), jnp.bfloat16),
            pltpu.VMEM((Z, 8, c.dz + c.tok), f32),
            pltpu.VMEM((G, 8, c.tok), f32),
            lanes(jnp.int32), lanes(f32), lanes(f32), lanes(f32), lanes(f32),
            pltpu.VMEM((8, c.tok), f32),
            pltpu.VMEM((c.resp, 8, c.tok), f32),
            pltpu.VMEM((G, 8, c.tok), f32),
            pltpu.VMEM((G, Z, 8, c.tok), f32),
            pltpu.VMEM((8, LANES), f32),
            pltpu.VMEM((c.resp, 8, LANES), f32),
            dma(2), pltpu.SemaphoreType.DMA, dma(DP), dma(G, Q, Z), dma(G, Q), dma(G, Q, Z), dma(G, Q, Z),
            dma(G, J), dma(G, J), dma(G, DP, J), dma(G, DP, J), dma(G, DP, J), dma(G, DP, J),
            dma(G), dma(G), dma(Z), dma(Z), dma(DP, F), dma(c.resp),
            dma(G, Z), dma(G, Z), dma(DP, F), dma(c.resp),
        ],
        compiler_params=pltpu.CompilerParams(
            collective_id=0, has_side_effects=True, vmem_limit_bytes=64 * 1024 * 1024 - 65536
        ),
    )(hidden, head_weight, tail, pack, ids, old_logp, advantages, lengths, rollout_row)
    return (new_logp, token_loss, summary[:3, 0])


def solution(mesh):
    rows = ("dp", "fsdp")
    in_specs = (
        P(rows, "tensor"), P("tensor"), P("fsdp", "tensor"), P(rows, None), P(rows),
        P(rows, None), P(rows, None), P(rows, "tensor"), P(rows),
    )
    out_specs = (P(rows, None), P(rows, None), P())
    return jax.shard_map(
        functools.partial(shards, functools.partial(Config, mesh)),
        mesh=mesh, in_specs=in_specs, out_specs=out_specs, check_vma=False,
    )
```

```python
import functools

import jax
import jax.numpy as jnp
from jax import lax
from jax.experimental import pallas as pl
from jax.experimental.pallas import tpu as pltpu
from jax.sharding import PartitionSpec as P

MESH = pl.DeviceIdType.MESH
clip_eps = 0.2
kl_coef = 0.2
log_limit = 10.0
norm_eps = 1e-06
LANES = 128
LOW = -1e30


def token_terms(new_logp, old_logp, advantages, ref_logp, live_mask, prob_square):
    shift = new_logp - old_logp
    prob_ratio = jnp.exp(jnp.clip(shift, -log_limit, log_limit))
    clipped = jnp.clip(prob_ratio, 1.0 - clip_eps, 1.0 + clip_eps)
    plain_term = prob_ratio * advantages
    bounded_term = clipped * advantages
    surrogate = jnp.minimum(plain_term, bounded_term)
    ref_gap = ref_logp - new_logp
    gap_clip = jnp.clip(ref_gap, -log_limit, log_limit)
    gap_exp = jnp.exp(gap_clip)
    kl_term = gap_exp - gap_clip - 1.0
    token_loss = live_mask * (kl_coef * kl_term - surrogate)
    gap_part = jnp.where(jnp.abs(ref_gap) < log_limit, kl_coef * (1.0 - gap_exp), 0.0)
    active = (plain_term <= bounded_term) & (jnp.abs(shift) < log_limit)
    grad_coef = live_mask * (gap_part - jnp.where(active, plain_term, 0.0))
    grad_square = grad_coef * grad_coef * (prob_square - 2.0 * jnp.exp(new_logp) + 1.0)
    return (token_loss, live_mask * kl_term, grad_square)


class Config:
    def __init__(self, mesh, tok, dz, kr, vt):
        self.dp, self.fs, self.tz = (mesh.shape[a] for a in ("dp", "fsdp", "tensor"))
        self.groups = self.fs // 2
        self.tok, self.dz, self.kr, self.vt = tok, dz, kr, vt
        self.dim = dz * self.tz
        tiles = -(-vt // LANES)
        self.half_tiles = -(-tiles // (self.groups * self.dp))
        self.half_cols = self.half_tiles * LANES
        self.block_cols = self.half_cols * self.dp
        self.pad_cols = self.block_cols * self.groups
        self.steps = 8
        self.rows = tok // self.steps
        self.chunk = 256 if self.half_cols % 256 == 0 else LANES
        self.wsteps = self.half_cols // self.chunk
        self.pairs = self.steps // 2
        self.pair_rows = 2 * self.rows
        self.resp = self.dp * self.fs


def kernel(
    c,
    hid, gain_in, w_any, id_in, roll_in, old_in, adv_in, len_in, row_in,
    out,
    pack_in, ids_in,
    x_buf, n_buf, w_own, w_full, packs, ids_all, rel, m_buf, l_buf, q_buf, p_buf,
    row_buf, roll, s_out, s_in, t_out, t_in,
    load_sem, x_sem, own_sem, tok_recv, y_send, right_send, left_send,
    wy_send, wy_recv, wx_send, wx_recv, core_send, core_recv,
    ids_send, ids_recv, pack_send, pack_recv, roll_send, roll_recv,
    st_send, st_recv, tot_send, tot_recv,
):
    G, Z, DP, F = c.groups, c.tz, c.dp, c.fs
    x = lax.axis_index("dp")
    f = lax.axis_index("fsdp")
    z = lax.axis_index("tensor")
    g, core = f // 2, f % 2
    partner = (x, g * 2 + (1 - core), z)
    me_resp = x * F + f
    pending = []

    def dev_g(gi):
        return (x, gi * 2 + core, z)

    def dev_x(xi):
        return (xi, f, z)

    def dev_z(zi):
        return (x, f, zi)

    def group(d):
        return lax.rem(g + d, G)

    def remote(src, dst, ss, rs, dev):
        return pltpu.make_async_remote_copy(
            src_ref=src, dst_ref=dst, send_sem=ss, recv_sem=rs, device_id=dev, device_id_type=MESH
        )

    def send(src, dst, ss, rs, dev, cond=None):
        copy = remote(src, dst, ss, rs, dev)
        if cond is None:
            copy.start()
        else:
            pl.when(cond)(copy.start)
        pending.append((cond, copy))

    def arrive(dst, rs, cond=None):
        copy = remote(dst, dst, rs, rs, partner)
        if cond is None:
            copy.wait_recv()
        else:
            pl.when(cond)(copy.wait_recv)

    load = pltpu.make_async_copy(w_any, w_own.at[pl.ds(0, c.vt), :], load_sem)
    load.start()
    zcols = pl.ds(pl.multiple_of(z * c.dz, c.dz), c.dz)
    own_x = pltpu.make_async_copy(hid, x_buf.at[g, :, zcols], x_sem)
    own_x.start()
    if c.vt < c.pad_cols:
        w_own[c.vt :, :] = jnp.zeros((c.pad_cols - c.vt, c.kr), w_own.dtype)
    part = roll_in.shape[1]
    pack_in[:, : c.dz] = jnp.broadcast_to(gain_in[...].astype(jnp.float32), (8, c.dz))
    pack_in[:, c.dz :] = jnp.zeros((8, c.tok), jnp.float32)
    for zi in range(Z):
        @pl.when(z == zi)
        def _(zi=zi):
            pack_in[:, c.dz + zi * part : c.dz + (zi + 1) * part] = jnp.broadcast_to(roll_in[...], (8, part))
    ids_in[...] = jnp.broadcast_to(id_in[...].astype(jnp.float32), (8, c.tok))

    barrier = pltpu.get_barrier_semaphore()
    count = 0
    for dg in range(G):
        for s in range(Z):
            if dg or s:
                pl.semaphore_signal(
                    barrier, inc=1,
                    device_id=(x, group(dg) * 2 + core, lax.rem(z + s, Z)), device_id_type=MESH,
                )
                count += 1
    for dx in range(DP):
        for df in range(F):
            if dx or df % 2:
                pl.semaphore_signal(
                    barrier, inc=1,
                    device_id=(lax.rem(x + dx, DP), lax.rem(f + df, F), z), device_id_type=MESH,
                )
                count += 1
    pl.semaphore_wait(barrier, count)

    def piece(gi, q, zi):
        return x_buf.at[
            gi, pl.ds(q * c.rows, c.rows), pl.ds(pl.multiple_of(zi * c.dz, c.dz), c.dz)
        ]

    def hid_piece(q):
        return hid.at[pl.ds(q * c.rows, c.rows), :]

    def w_block(fi, h, j):
        return w_full.at[
            pl.ds(pl.multiple_of(h * c.half_cols + j * c.chunk, c.chunk), c.chunk),
            pl.ds(pl.multiple_of(fi * c.kr, c.kr), c.kr),
        ]

    def own_block(gi, h, j):
        start = gi * c.block_cols + h * c.half_cols + j * c.chunk
        return w_own.at[pl.ds(pl.multiple_of(start, c.chunk), c.chunk), :]

    def y_tokens(q):
        for d in range(1, G):
            send(hid_piece(q), piece(g, q, z), y_send.at[d, q], tok_recv.at[g, q, z], dev_g(group(d)))

    def y_weights(j):
        for d in range(1, G):
            gi = group(d)
            send(own_block(gi, x, j), w_block(f, x, j), wy_send.at[d, j], wy_recv.at[g, j], dev_g(gi))

    def z_move(q, s):
        right_ok = z - s >= 0
        left_ok = z + s < Z
        zr = jnp.maximum(z - s, 0)
        zl = jnp.minimum(z + s, Z - 1)
        for d in range(G):
            gi = group(d)
            if s == 0:
                if d:
                    arrive(piece(gi, q, z), tok_recv.at[gi, q, z])
                src_r = src_l = hid_piece(q) if d == 0 else piece(gi, q, z)
            else:
                arrive(piece(gi, q, zr), tok_recv.at[gi, q, zr], right_ok)
                arrive(piece(gi, q, zl), tok_recv.at[gi, q, zl], left_ok)
                src_r, src_l = piece(gi, q, zr), piece(gi, q, zl)
            if s < Z - 1:
                send(src_r, piece(gi, q, zr), right_send.at[gi, q, zr], tok_recv.at[gi, q, zr],
                     dev_z(jnp.minimum(z + 1, Z - 1)), right_ok & (z + 1 < Z))
                send(src_l, piece(gi, q, zl), left_send.at[gi, q, zl], tok_recv.at[gi, q, zl],
                     dev_z(jnp.maximum(z - 1, 0)), left_ok & (z >= 1))

    def core_pass(src, fi, h, j):
        gi = fi // 2
        send(src, w_block(fi, h, j), core_send.at[gi, h, j], core_recv.at[gi, h, j], partner)

    for d in range(1, G):
        send(ids_in, ids_all.at[g], ids_send.at[d], ids_recv.at[g], dev_g(group(d)))
    for s in range(1, Z):
        send(pack_in, packs.at[z], pack_send.at[s], pack_recv.at[z], dev_z(lax.rem(z + s, Z)))
    y_tokens(0)

    m_buf[...] = jnp.full(m_buf.shape, LOW, jnp.float32)
    for ref in (l_buf, q_buf, p_buf):
        ref[...] = jnp.zeros(ref.shape, jnp.float32)
    packs[z] = pack_in[...]
    ids_all[g] = ids_in[...]
    load.wait()
    y_weights(0)
    own_copies = []
    for h in range(DP):
        start = pl.multiple_of(g * c.block_cols + h * c.half_cols, LANES)
        copy = pltpu.make_async_copy(
            w_own.at[pl.ds(start, c.half_cols), :],
            w_full.at[pl.ds(h * c.half_cols, c.half_cols), pl.ds(pl.multiple_of(f * c.kr, c.kr), c.kr)],
            own_sem.at[h],
        )
        copy.start()
        own_copies.append(copy)

    def normalize(q):
        rows = pl.ds(q * c.rows, c.rows)
        for gi in range(G):
            values = x_buf[gi, rows, :].astype(jnp.float32)
            inv = lax.rsqrt(jnp.sum(values * values, axis=1, keepdims=True) / c.dim + norm_eps)
            for zi in range(Z):
                gain = packs[zi, 0:1, 0:c.dz]
                part = values[:, zi * c.dz : (zi + 1) * c.dz]
                n_buf[gi, rows, zi * c.dz : (zi + 1) * c.dz] = (part * inv * gain).astype(jnp.bfloat16)

    def unit(p, start, size):
        rows = pl.ds(pl.multiple_of(p * c.pair_rows, c.pair_rows), c.pair_rows)
        width = G * c.pair_rows
        for h in range(DP):
            off = h * c.half_cols + start
            cols = pl.ds(pl.multiple_of(off, c.chunk), size)
            tokens = jnp.concatenate([n_buf[gi, rows, :] for gi in range(G)], axis=0)
            logits = lax.dot_general(
                w_full[cols, :], tokens, (((1,), (1,)), ((), ())), preferred_element_type=jnp.float32
            ).reshape(size // 8, 8, width)
            valid = c.vt - g * c.block_cols - off
            place = rel[p] - off
            index = lax.broadcasted_iota(jnp.int32, (size // 8, 8, 1), 0) * 8 + lax.broadcasted_iota(
                jnp.int32, (size // 8, 8, 1), 1
            )
            p_buf[p] = p_buf[p] + jnp.sum(jnp.where(index == place[None], logits, 0.0), axis=0)
            logits = jnp.where(index < valid, logits, LOW)
            before = m_buf[p]
            top = jnp.maximum(before, jnp.max(logits, axis=0))
            scale = jnp.exp(before - top)
            e = jnp.exp(logits - top[None])
            m_buf[p] = top
            l_buf[p] = l_buf[p] * scale + jnp.sum(e, axis=0)
            q_buf[p] = q_buf[p] * (scale * scale) + jnp.sum(e * e, axis=0)

    for i in range(c.steps + Z - 1):
        if i + 1 < c.steps:
            y_tokens(i + 1)
        if i + 1 < c.wsteps:
            y_weights(i + 1)
        if i < c.wsteps:
            for h in range(DP):
                core_pass(own_block(g, h, i), f, h, i)
        if i < c.steps:
            z_move(i, 0)
        if 0 <= i - 1 < c.wsteps:
            j = i - 1
            for d in range(1, G):
                gi = group(d)
                fi = gi * 2 + core
                arrive(w_block(fi, x, j), wy_recv.at[gi, j])
                for dx in range(1, DP):
                    xi = lax.rem(x + dx, DP)
                    send(w_block(fi, x, j), w_block(fi, x, j), wx_send.at[gi, dx, j],
                         wx_recv.at[gi, x, j], dev_x(xi))
                core_pass(w_block(fi, x, j), fi, x, j)
        for s in range(1, Z - 1):
            if 0 <= i - s < c.steps:
                z_move(i - s, s)
        if 0 <= i - 2 < c.wsteps:
            j = i - 2
            for d in range(1, G):
                gi = group(d)
                fi = gi * 2 + core
                for dx in range(1, DP):
                    xi = lax.rem(x + dx, DP)
                    arrive(w_block(fi, xi, j), wx_recv.at[gi, xi, j])
                    core_pass(w_block(fi, xi, j), fi, xi, j)
        if i == 1:
            for s in range(1, Z):
                zi = lax.rem(z + s, Z)
                arrive(packs.at[zi], pack_recv.at[zi])
            row_buf[...] = sum(packs[zi, :, c.dz :] for zi in range(Z))
            for d in range(1, G):
                arrive(ids_all.at[group(d)], ids_recv.at[group(d)])
            base = z * c.vt + g * c.block_cols
            for p in range(c.pairs):
                for gi in range(G):
                    ids = ids_all[gi, :, p * c.pair_rows : (p + 1) * c.pair_rows]
                    rel[p, :, gi * c.pair_rows : (gi + 1) * c.pair_rows] = ids.astype(jnp.int32) - base
            own_x.wait()
            for copy in own_copies:
                copy.wait()
        if i == 2:
            for dx in range(DP):
                for df in range(F):
                    if dx or df:
                        xi, fi = lax.rem(x + dx, DP), lax.rem(f + df, F)
                        send(row_buf, roll.at[me_resp], roll_send.at[dx, df], roll_recv.at[me_resp],
                             (xi, fi, z))
        q = i - (Z - 1)
        if q >= 0:
            if q < c.wsteps:
                for gi in range(G):
                    for h in range(DP):
                        arrive(w_block(gi * 2 + 1 - core, h, q), core_recv.at[gi, h, q])
                p = q // 2
                if q % 2 or q == c.wsteps - 1:
                    first = q - q % 2
                    if p:
                        pl.loop(0, p)(lambda pp, q=q, first=first: unit(pp, first * c.chunk, (q + 1 - first) * c.chunk))
            z_move(q, Z - 1)
            normalize(q)
            if q % 2:
                ready = min(q + 1, c.wsteps)
                span = min(2, ready)
                pl.loop(0, ready // span)(lambda jj, q=q, span=span: unit(q // 2, jj * (span * c.chunk), span * c.chunk))

    s_out[...] = jnp.zeros(s_out.shape, jnp.float32)
    for p in range(c.pairs):
        m_p = m_buf[p]
        top = jnp.max(m_p, axis=0, keepdims=True)
        scale = jnp.exp(m_p - top)
        total = jnp.sum(l_buf[p] * scale, axis=0, keepdims=True)
        square = jnp.sum(q_buf[p] * (scale * scale), axis=0, keepdims=True)
        picked = jnp.sum(p_buf[p], axis=0, keepdims=True)
        for gi in range(G):
            here = slice(gi * c.pair_rows, (gi + 1) * c.pair_rows)
            there = slice(p * c.pair_rows, (p + 1) * c.pair_rows)
            for k, value in enumerate((top, total, square, picked)):
                s_out[gi, k : k + 1, there] = value[:, here]
    for s in range(Z - 1, -1, -1):
        for d in range(G):
            if s or d:
                gi, zi = group(d), lax.rem(z + s, Z)
                send(s_out.at[gi], s_in.at[g, z], st_send.at[d, s], st_recv.at[g, z],
                     (x, gi * 2 + core, zi))
    s_in[g, z] = s_out[g]

    roll[me_resp] = row_buf[...]
    for dx in range(DP):
        for df in range(F):
            if dx or df:
                r = lax.rem(x + dx, DP) * F + lax.rem(f + df, F)
                arrive(roll.at[r], roll_recv.at[r])
    ref = jnp.zeros((1, c.tok), jnp.float32)
    for r in range(c.resp):
        ref = ref + jnp.where(row_in[0] == r, roll[r, 0:1, :], 0.0)
    position = lax.broadcasted_iota(jnp.int32, (1, c.tok), 1)
    live = jnp.where(position < len_in[0], 1.0, 0.0)

    for s in range(Z):
        for d in range(G):
            if s or d:
                gi, zi = group(d), lax.rem(z + s, Z)
                arrive(s_in.at[gi, zi], st_recv.at[gi, zi])
    every = [(gi, zi) for gi in range(G) for zi in range(Z)]
    top = s_in[0, 0, 0:1, :]
    for gi, zi in every[1:]:
        top = jnp.maximum(top, s_in[gi, zi, 0:1, :])
    total = square = picked = jnp.zeros((1, c.tok), jnp.float32)
    for gi, zi in every:
        scale = jnp.exp(s_in[gi, zi, 0:1, :] - top)
        total = total + s_in[gi, zi, 1:2, :] * scale
        square = square + s_in[gi, zi, 2:3, :] * (scale * scale)
        picked = picked + s_in[gi, zi, 3:4, :]
    new_logp = picked - top - jnp.log(total)
    prob_square = square / (total * total)
    token_loss, kl_part, grad_part = token_terms(
        new_logp, old_in[...], adv_in[...], ref, live, prob_square
    )
    sums = [jnp.sum(v, axis=1, keepdims=True) for v in (live, token_loss, kl_part, grad_part)]
    t_out[...] = jnp.concatenate(
        [jnp.broadcast_to(v, (1, LANES)) for v in sums] + [jnp.zeros((4, LANES), jnp.float32)], axis=0
    )
    for dx in range(DP):
        for df in range(F):
            if dx or df:
                xi, fi = lax.rem(x + dx, DP), lax.rem(f + df, F)
                send(t_out, t_in.at[me_resp], tot_send.at[dx, df], tot_recv.at[me_resp], (xi, fi, z))
    t_in[me_resp] = t_out[...]
    out[0:1, :] = new_logp
    out[1:2, :] = token_loss
    for dx in range(DP):
        for df in range(F):
            if dx or df:
                r = lax.rem(x + dx, DP) * F + lax.rem(f + df, F)
                arrive(t_in.at[r], tot_recv.at[r])
    totals = sum(t_in[r] for r in range(c.resp))
    count = totals[0:1]
    for k, value in enumerate((totals[1:2] / count, totals[2:3] / count, jnp.sqrt(totals[3:4] / count))):
        out[2 + k : 3 + k, :] = jnp.broadcast_to(value[:, 0:1], (1, c.tok))
    out[5:8, :] = jnp.zeros((3, c.tok), jnp.float32)
    for cond, copy in pending:
        if cond is None:
            copy.wait_send()
        else:
            pl.when(cond)(copy.wait_send)


def shards(c_of, hidden, norm_gain, head_weight, token_ids, lengths, old_logp, advantages, rollout_logp, rollout_row):
    c = c_of(hidden.shape[0], hidden.shape[1], head_weight.shape[0], head_weight.shape[1])
    G, Z, DP, F = c.groups, c.tz, c.dp, c.fs
    vmem = pl.BlockSpec(memory_space=pltpu.VMEM)
    smem = pl.BlockSpec(memory_space=pltpu.SMEM)
    hbm = pl.BlockSpec(memory_space=pl.ANY)
    dma = lambda *shape: pltpu.SemaphoreType.DMA(shape)
    f32 = jnp.float32
    lanes = lambda dtype: pltpu.VMEM((c.pairs, 8, G * c.pair_rows), dtype)
    Q, J = c.steps, c.wsteps
    out = pl.pallas_call(
        functools.partial(kernel, c),
        out_shape=jax.ShapeDtypeStruct((8, c.tok), f32),
        in_specs=[vmem, vmem, hbm, vmem, vmem, vmem, vmem, smem, smem],
        out_specs=vmem,
        scratch_shapes=[
            pltpu.VMEM((8, c.dz + c.tok), f32),
            pltpu.VMEM((8, c.tok), f32),
            pltpu.VMEM((G, c.tok, c.dim), jnp.bfloat16),
            pltpu.VMEM((G, c.tok, c.dim), jnp.bfloat16),
            pltpu.VMEM((c.pad_cols, c.kr), jnp.bfloat16),
            pltpu.VMEM((c.block_cols, c.dim), jnp.bfloat16),
            pltpu.VMEM((Z, 8, c.dz + c.tok), f32),
            pltpu.VMEM((G, 8, c.tok), f32),
            lanes(jnp.int32), lanes(f32), lanes(f32), lanes(f32), lanes(f32),
            pltpu.VMEM((8, c.tok), f32),
            pltpu.VMEM((c.resp, 8, c.tok), f32),
            pltpu.VMEM((G, 8, c.tok), f32),
            pltpu.VMEM((G, Z, 8, c.tok), f32),
            pltpu.VMEM((8, LANES), f32),
            pltpu.VMEM((c.resp, 8, LANES), f32),
            pltpu.SemaphoreType.DMA, pltpu.SemaphoreType.DMA, dma(DP), dma(G, Q, Z), dma(G, Q), dma(G, Q, Z), dma(G, Q, Z),
            dma(G, J), dma(G, J), dma(G, DP, J), dma(G, DP, J), dma(G, DP, J), dma(G, DP, J),
            dma(G), dma(G), dma(Z), dma(Z), dma(DP, F), dma(c.resp),
            dma(G, Z), dma(G, Z), dma(DP, F), dma(c.resp),
        ],
        compiler_params=pltpu.CompilerParams(
            collective_id=0, has_side_effects=True, vmem_limit_bytes=64 * 1024 * 1024 - 65536
        ),
    )(hidden, norm_gain[None, :], head_weight.T, token_ids, rollout_logp, old_logp, advantages, lengths, rollout_row)
    return (out[0:1], out[1:2], out[2:5, 0])


def solution(mesh):
    rows = ("dp", "fsdp")
    in_specs = (
        P(rows, "tensor"), P("tensor"), P("fsdp", "tensor"), P(rows, None), P(rows),
        P(rows, None), P(rows, None), P(rows, "tensor"), P(rows),
    )
    out_specs = (P(rows, None), P(rows, None), P())
    return jax.shard_map(
        functools.partial(shards, functools.partial(Config, mesh)),
        mesh=mesh, in_specs=in_specs, out_specs=out_specs, check_vma=False,
    )
```
